32 devices in a mesh: rows: 8 (over z, y), cols: 4 (over x, core).
Axes of the slice: x: 2, y: 2, z: 4, core: 2. Of those that a mesh axis runs over, the one named last changes fastest.
Arguments:
- blocks: bfloat16 [32, 4, 3, 128, 128], P('rows', 'cols'), may hold values from -1.1953125 to 1.1953125
- block_cols: int32 [32, 4, 3], P('rows', 'cols'), may hold values from 0 to 31, as said below
Outputs:
- square_blocks: bfloat16 [32, 4, 36, 128, 128], P('rows', 'cols')
- square_cols: int32 [32, 4, 36], P('rows', 'cols')
- square_start: int32 [32, 4], P('rows', 'cols')
The draws below stay inside these ranges and needn't reach their ends.
Inputs may be any that keep to these rules, and one draw needn't show every extreme that they name: Block-row i lies in panel p = i // 4; every block_cols[i, g, s] is a block-column congruent to g modulo 4 among block-rows 4 * (p - 4) to 4 * (p + 4) - 1, taken modulo 32; the three entries of one group differ; the block-columns i - 1, i and i + 1 (modulo 32) are always among a row's entries.
All inputs are finite; a program needn't handle non-finite values.
Results may differ from the reference program's by a relative error of at most 0.001.
Values may be sent and summed in bfloat16 or wider, within the bound.
A program may use at most 64 MiB of HBM per device.

```python
import jax
import jax.numpy as jnp
from jax import lax

BS = 128
PB = 4
KG = 3
HP = 4
GROUPS = 4
NB = 32
K = 12


def draw_block_cols(key, part):
    row_ids = jnp.arange(NB, dtype=jnp.int32)
    panel = row_ids // PB
    window_base = (panel - HP) * PB % NB
    choices_count = 2 * HP * PB // GROUPS
    group_ids = jnp.arange(GROUPS, dtype=jnp.int32)
    residue = (group_ids[None, :] - window_base[:, None]) % GROUPS
    delta = (group_ids[None, :] - row_ids[:, None] + 1) % GROUPS
    has_band = delta <= 2
    band_col = (row_ids[:, None] - 1 + delta) % NB
    band_place = (band_col - window_base[:, None]) % NB // GROUPS
    key_pick = jax.random.fold_in(key, 11)
    key_jump = jax.random.fold_in(key, 23)
    key_extra = jax.random.fold_in(key, 37)
    picked = jax.random.randint(key_pick, (NB, GROUPS), 0, choices_count, dtype=jnp.int32)
    jumped = jax.random.randint(key_jump, (NB, GROUPS), 1, choices_count, dtype=jnp.int32)
    extra = jax.random.randint(key_extra, (NB, GROUPS), 1, choices_count - 1, dtype=jnp.int32)
    other_jump = 1 + (jumped - 1 + extra) % (choices_count - 1)
    first_place = jnp.where(has_band, band_place, picked)
    second_place = (first_place + jumped) % choices_count
    third_place = (first_place + other_jump) % choices_count
    first_col = (window_base[:, None] + first_place * GROUPS + residue) % NB
    second_col = (window_base[:, None] + second_place * GROUPS + residue) % NB
    third_col = (window_base[:, None] + third_place * GROUPS + residue) % NB
    return jnp.stack([first_col, second_col, third_col], axis=-1).astype(jnp.int32)


def steps_of(stream_key, shape, shards, low, high):
    level = 1.0
    for axis_at, shards_of in shards:
        draws = jax.random.uniform(jax.random.fold_in(jax.random.fold_in(stream_key, 6), axis_at), (shards_of,), jnp.float32, low / len(shards), high / len(shards))
        level = level * jnp.repeat(jnp.exp(draws), shape[axis_at] // shards_of).reshape((-1,) + (1,) * (len(shape) - 1 - axis_at))
    return level


def centred(rng, shape, deviation, bound, shards=(), kind=jnp.bfloat16):
    result = deviation * jax.random.normal(rng, shape, jnp.float32)
    if shards:
        result = result * steps_of(rng, shape, shards, -0.22, 0.18)
    return jnp.clip(result, -bound, bound).astype(kind)


def setup_inputs(seed: int = 0) -> dict:
    key_of = jax.random.split(jax.random.key(seed), 3)
    blocks = centred(key_of[0], (NB, GROUPS, KG, BS, BS), 0.2, 1.1953125, ((0, 8), (1, 4)))
    block_cols = draw_block_cols(jax.random.fold_in(key_of[2], 71), 0)
    return dict(blocks=blocks, block_cols=block_cols)


def unique_slots(candidates):
    width = candidates.shape[-1]
    ordered = jnp.sort(candidates, axis=-1)
    firsts = jnp.concatenate([jnp.ones(ordered.shape[:-1] + (1,), dtype=bool), ordered[..., 1:] != ordered[..., :-1]], axis=-1)
    marks = firsts.astype(jnp.int32)
    totals = jnp.sum(marks, axis=-1).astype(jnp.int32)
    ranking = jnp.sum(marks[..., None, :] * (ordered[..., None, :] < candidates[..., :, None]).astype(jnp.int32), axis=-1)
    places = jnp.cumsum(marks, axis=-1) - 1
    slot_ids = jnp.arange(width, dtype=jnp.int32)
    chosen = (places[..., None, :] == slot_ids[:, None]) & firsts[..., None, :]
    columns = jnp.sum(jnp.where(chosen, ordered[..., None, :], 0), axis=-1).astype(jnp.int32)
    columns = jnp.where(slot_ids < totals[..., None], columns, -1).astype(jnp.int32)
    onehot = (ranking[..., None, :] == slot_ids[:, None]).astype(jnp.float32)
    return columns, onehot, totals


def reference(blocks, block_cols):
    def one_row(row_index):
        named = block_cols[row_index].reshape(K).astype(jnp.int32)
        left = blocks[row_index].reshape(K, BS, BS).astype(jnp.float32)
        right_vals = blocks[named].astype(jnp.float32)
        right_cols = block_cols[named]
        products = jnp.einsum("tab,tgsbc->gtsac", left, right_vals, precision=lax.Precision.HIGHEST)
        candidates = jnp.transpose(right_cols, (1, 0, 2)).reshape(GROUPS, K * KG)
        columns, onehot, totals = unique_slots(candidates)
        merged = jnp.einsum("goq,gqac->goac", onehot, products.reshape(GROUPS, K * KG, BS, BS), precision=lax.Precision.HIGHEST)
        return merged.astype(jnp.bfloat16), columns, totals

    square_blocks, square_cols, counts = lax.map(one_row, jnp.arange(NB, dtype=jnp.int32))
    square_start = (jnp.cumsum(counts, axis=0) - counts).astype(jnp.int32)
    return square_blocks, square_cols, square_start
```

```python
import functools

import jax
import jax.numpy as jnp
from jax import lax
from jax.experimental import pallas as pl
from jax.experimental.pallas import tpu as pltpu
from jax.sharding import PartitionSpec as P

HP = 4


def shifted(block, axis, distance):
    devices = range(lax.axis_size(axis))
    route = [((i - distance) % len(devices), i) for i in devices]
    return lax.ppermute(block, axis, route)


def unique_slots(candidates):
    width = candidates.shape[-1]
    ordered = jnp.sort(candidates, axis=-1)
    firsts = jnp.concatenate(
        [jnp.ones(ordered.shape[:-1] + (1,), dtype=bool), ordered[..., 1:] != ordered[..., :-1]],
        axis=-1,
    )
    marks = firsts.astype(jnp.int32)
    totals = jnp.sum(marks, axis=-1)
    ranking = jnp.sum(
        marks[..., None, :] * (ordered[..., None, :] < candidates[..., :, None]).astype(jnp.int32),
        axis=-1,
    )
    places = jnp.cumsum(marks, axis=-1) - 1
    slot_ids = jnp.arange(width, dtype=jnp.int32)
    chosen = (places[..., None, :] == slot_ids[:, None]) & firsts[..., None, :]
    columns = jnp.sum(jnp.where(chosen, ordered[..., None, :], 0), axis=-1).astype(jnp.int32)
    columns = jnp.where(slot_ids < totals[..., None], columns, -1)
    onehot = (ranking[..., None, :] == slot_ids[:, None]).astype(jnp.float32)
    return (columns, onehot, totals)


def on_device(blocks, block_cols):
    panel_rows = block_cols.shape[0]
    per_group = block_cols.shape[2]
    block_size = blocks.shape[-1]
    cycle_size = lax.axis_size("rows")
    block_rows = panel_rows * cycle_size
    panel_id = lax.axis_index("rows")
    left_vals, left_cols = (
        lax.all_gather(blocks, "cols", axis=1, tiled=True),
        lax.all_gather(block_cols, "cols", axis=1, tiled=True),
    )
    groups = left_cols.shape[1]
    row_slots = groups * per_group
    left_vals = left_vals.reshape(panel_rows, row_slots, block_size, block_size)
    left_cols = left_cols.reshape(panel_rows, row_slots)
    own_panel = (blocks[:, 0], block_cols[:, 0])
    pieces = []
    for offset in range(-HP, HP):
        if offset == 0:
            pieces.append(own_panel)
        else:
            pieces.append(shifted((own_panel[0], own_panel[1]), "rows", -offset))
    win_vals = jnp.concatenate([piece[0] for piece in pieces], axis=0)
    win_cols = jnp.concatenate([piece[1] for piece in pieces], axis=0)
    window_base = (panel_id - HP) * panel_rows % block_rows
    local_index = ((left_cols - window_base) % block_rows).astype(jnp.int32)
    right_vals = win_vals[local_index]
    right_cols = win_cols[local_index]
    products = jnp.einsum(
        "ptab,ptsbc->ptsac", left_vals, right_vals, preferred_element_type=jnp.float32
    )
    candidates = right_cols.reshape(panel_rows, row_slots * per_group)
    columns, onehot, totals = unique_slots(candidates)
    merged = jnp.einsum(
        "poq,pqac->poac",
        onehot,
        products.reshape(panel_rows, row_slots * per_group, block_size, block_size),
        precision=lax.Precision.HIGHEST,
    )
    merged_blocks = merged.astype(jnp.bfloat16)
    panel_total = jnp.sum(totals)
    all_totals = lax.all_gather(panel_total.reshape(1), "rows", axis=0, tiled=True)
    earlier = jnp.sum(jnp.where(jnp.arange(cycle_size, dtype=jnp.int32) < panel_id, all_totals, 0))
    starts = earlier + jnp.cumsum(totals) - totals
    return (merged_blocks[:, None], columns[:, None], starts[:, None])


NY = 2
SPANS = (2, 5, 5)
FILL = 1
CROSS = 1
VMEM_LIMIT = 16 * 1024 * 1024


def popcount(x, width):
    total = x & 1
    for b in range(1, width):
        total = total + ((x >> b) & 1)
    return total


def gather_kernel(
    sizes, own_ref, own_cols_ref, win_ref, left_ref, meta_ref,
    cols_buf, cols_smem, mask_smem,
    recv_sem, send_sem, crecv_sem, csend_sem, prow_recv, prow_send,
    lrecv_sem, lsend_sem, local_sem,
):
    R, C, PB, KG = sizes
    Z = R // NY
    CHUNKS = len(SPANS)
    begins = [sum(SPANS[:q]) for q in range(CHUNKS)]
    r = lax.axis_index("rows")
    c = lax.axis_index("cols")
    z, y = r // NY, r % NY
    other_y = 1 - y
    core_peer = (c // 2) * 2 + (1 - c % 2)
    x_peer = (c + 2) % C
    y_row = z * NY + other_y
    up_row, down_row = (z + 1) * NY + y, (z - 1) * NY + y
    has_up, has_down = z < Z - 1, z > 0
    UP, DOWN, SIDE = 0, 1, 2
    targets = {UP: up_row, DOWN: down_row, SIDE: y_row}

    local = [
        pltpu.make_async_copy(own_ref, win_ref.at[r], local_sem.at[0]),
        pltpu.make_async_copy(own_ref, left_ref.at[c], local_sem.at[1]),
        pltpu.make_async_copy(own_cols_ref, cols_buf.at[r, c], local_sem.at[2]),
    ]

    barrier = pltpu.get_barrier_semaphore()
    for cp in local:
        cp.start()

    def greet(rr, cc):
        pl.semaphore_signal(barrier, inc=1, device_id=(rr, cc), device_id_type=pl.DeviceIdType.MESH)

    greet(y_row, c)
    for d in range(1, C):
        greet(r, (c + d) % C)
    pl.when(has_up)(lambda: greet(up_row, c))
    pl.when(has_down)(lambda: greet(down_row, c))
    pl.semaphore_wait(barrier, C + jnp.minimum(z, 1) + jnp.minimum(Z - 1 - z, 1))

    def part(ref, row, chunk):
        return ref.at[row, pl.ds(begins[chunk], SPANS[chunk])]

    def chunk_copy(way, row, chunk):
        src = part(win_ref, row, chunk)
        return pltpu.make_async_remote_copy(
            src_ref=src, dst_ref=part(win_ref, row, chunk),
            send_sem=send_sem.at[way, row, chunk], recv_sem=recv_sem.at[row, chunk],
            device_id=(targets[way], c), device_id_type=pl.DeviceIdType.MESH,
        )

    def prow_copy(way, row):
        return pltpu.make_async_remote_copy(
            src_ref=cols_buf.at[row], dst_ref=cols_buf.at[row],
            send_sem=prow_send.at[way, row], recv_sem=prow_recv.at[row],
            device_id=(targets[way], c), device_id_type=pl.DeviceIdType.MESH,
        )

    def cols_copy(cc, group, d):
        return pltpu.make_async_remote_copy(
            src_ref=cols_buf.at[r, group], dst_ref=cols_buf.at[r, group],
            send_sem=csend_sem.at[d], recv_sem=crecv_sem.at[group],
            device_id=(r, cc), device_id_type=pl.DeviceIdType.MESH,
        )

    def left_copy(cc, group, d):
        return pltpu.make_async_remote_copy(
            src_ref=left_ref.at[group], dst_ref=left_ref.at[group],
            send_sem=lsend_sem.at[d], recv_sem=lrecv_sem.at[group],
            device_id=(r, cc), device_id_type=pl.DeviceIdType.MESH,
        )

    def both(act):
        pl.when(has_up)(lambda: act(UP))
        pl.when(has_down)(lambda: act(DOWN))

    def send_own(chunks):
        def act(way):
            for q in chunks:
                chunk_copy(way, r, q).start()
        both(act)

    local[2].wait()
    for d in range(1, C):
        cols_copy((c + d) % C, c, d).start()
    local[0].wait()
    cross = list(range(CROSS))
    rest = list(range(CROSS, CHUNKS))

    def send_side(chunks):
        for q in chunks:
            chunk_copy(SIDE, r, q).start()

    send_side(cross)
    send_own(rest[:1])
    send_side(rest[:1])
    for d in range(1, C):
        cols_copy(c, (c + d) % C, d).wait_recv()

    both(lambda way: prow_copy(way, r).start())
    prow_copy(SIDE, r).start()
    send_own(rest[1:])
    send_side(rest[1:])
    local[1].wait()
    left_copy(x_peer, c, 0).start()
    left_copy(core_peer, c, 1).start()

    def from_planes(d, act):
        @pl.when(z >= d)
        def _():
            act(z - d, UP, has_up)

        @pl.when(z + d < Z)
        def _():
            act(z + d, DOWN, has_down)

    def pass_prow(plane, way, more):
        row = plane * NY + y
        prow_copy(way, row).wait_recv()
        pl.when(more)(lambda: prow_copy(way, row).start())
        prow_copy(SIDE, row).start()

    def pass_chunk(q):
        def act(plane, way, more):
            row = plane * NY + y
            chunk_copy(way, row, q).wait_recv()
            pl.when(more)(lambda: chunk_copy(way, row, q).start())
            chunk_copy(SIDE, row, q).start()
        return act

    def pass_cross(q, line):
        def act(plane, way, more):
            @pl.when(more)
            def _():
                chunk_copy(way, plane * NY + line, q).wait_recv()
                chunk_copy(way, plane * NY + line, q).start()
        return act

    def take_cross(q, line):
        def act(plane, way, more):
            pl.when(jnp.logical_not(more))(
                lambda: chunk_copy(way, plane * NY + line, q).wait_recv()
            )
        return act

    def cross_planes(act):
        for d in range(1, Z):
            for line in (y, other_y):
                for q in cross:
                    from_planes(d, act(q, line))

    for d in range(1, Z):
        for n, q in enumerate(rest):
            from_planes(d, pass_chunk(q))
            if n == 0:
                from_planes(d, pass_prow)
        if d == FILL:
            send_own(cross)
            for q in cross:
                chunk_copy(SIDE, y_row, q).wait_recv()
                both(lambda way: chunk_copy(way, y_row, q).start())
        if d == 1:
            left_copy(c, x_peer, 0).wait_recv()
            left_copy(core_peer, x_peer, 2).start()
    cross_planes(pass_cross)

    def each_plane(act):
        for d in range(1, Z):
            from_planes(d, lambda plane, way, more: act(plane))

    prow_copy(SIDE, y_row).wait_recv()
    each_plane(lambda plane: prow_copy(SIDE, plane * NY + other_y).wait_recv())
    to_smem = pltpu.make_async_copy(cols_buf, cols_smem, local_sem.at[3])
    to_smem.start()
    to_smem.wait()

    def fill_mask(rr, carry):
        for i in range(PB):
            m = jnp.int32(0)
            for s in range(KG):
                m = m | (jnp.int32(1) << (cols_smem[rr, c, s, 0, i] // C))
            mask_smem[rr * PB + i] = m
        return carry

    lax.fori_loop(0, R, fill_mask, jnp.int32(0))
    classes = R * PB // C

    def row_mask(rr, i):
        m = jnp.int32(0)
        for g in range(C):
            for s in range(KG):
                m = m | mask_smem[cols_smem[rr, g, s, 0, i]]
        return m

    def count_panel(rr, total):
        for i in range(PB):
            total = total + popcount(row_mask(rr, i), classes)
        return total

    start = lax.fori_loop(0, r, count_panel, jnp.int32(0))
    base = PB * C * KG * KG
    for i in range(PB):
        m = row_mask(r, i)
        meta_ref[base + PB * C * KG + i] = m
        meta_ref[base + PB * C * KG + PB + i] = start
        ranks = jnp.int32(0)
        rank = jnp.int32(0)
        for a in range(classes):
            ranks = ranks | (rank << (4 * a))
            rank = rank + ((m >> a) & 1)
        start = start + rank
        for g in range(C):
            for s in range(KG):
                e = g * KG + s
                k = cols_smem[r, g, s, 0, i]
                meta_ref[base + i * C * KG + e] = k
                for t in range(KG):
                    a = cols_smem[k // PB, c, t, 0, k % PB] // C
                    meta_ref[(i * C * KG + e) * KG + t] = (ranks >> (4 * a)) & 15

    cross_planes(take_cross)
    for q in rest:
        chunk_copy(SIDE, y_row, q).wait_recv()
        each_plane(lambda plane: chunk_copy(SIDE, plane * NY + other_y, q).wait_recv())
    left_copy(c, core_peer, 1).wait_recv()
    left_copy(c, (core_peer + 2) % C, 2).wait_recv()

    for d in range(1, C):
        cols_copy((c + d) % C, c, d).wait_send()
    left_copy(x_peer, c, 0).wait_send()
    left_copy(core_peer, c, 1).wait_send()
    left_copy(core_peer, x_peer, 2).wait_send()
    for q in range(CHUNKS):
        chunk_copy(SIDE, r, q).wait_send()
        both(lambda way: chunk_copy(way, r, q).wait_send())
        if q in cross:
            both(lambda way: chunk_copy(way, y_row, q).wait_send())
    both(lambda way: prow_copy(way, r).wait_send())
    prow_copy(SIDE, r).wait_send()

    def sent(plane, way, more):
        row = plane * NY + y
        prow_copy(SIDE, row).wait_send()
        for q in rest:
            chunk_copy(SIDE, row, q).wait_send()

        @pl.when(more)
        def _():
            prow_copy(way, row).wait_send()
            for q in range(CHUNKS):
                chunk_copy(way, row, q).wait_send()
            for q in cross:
                chunk_copy(way, plane * NY + other_y, q).wait_send()

    for d in range(1, Z):
        from_planes(d, sent)


def square_kernel(
    sizes, meta_ref, left_ref, win_ref, out_ref, cols_ref, start_ref,
    acc, zeros, rows, cols_smem, start_smem, row_sem, fill_sem, small_sem,
):
    R, C, PB, KG = sizes
    me = lax.axis_index("cols")
    slots = C * KG * KG
    classes = R * PB // C
    base = PB * slots
    zeros[...] = jnp.zeros_like(zeros)

    def fill(i):
        return pltpu.make_async_copy(
            zeros, out_ref.at[i, 0, pl.ds(classes, slots - classes)], fill_sem.at[i]
        )

    def store(i):
        return pltpu.make_async_copy(
            rows.at[i], out_ref.at[i, 0, pl.ds(0, classes)], row_sem.at[i]
        )

    for i in range(PB):
        fill(i).start()
    for i in range(PB):
        m = meta_ref[base + PB * C * KG + i]
        start_smem[0, i] = meta_ref[base + PB * C * KG + PB + i]
        for o in range(slots):
            cols_smem[i, 0, o] = -1
        rank = jnp.int32(0)
        for a in range(classes):
            bit = (m >> a) & 1
            cols_smem[i, 0, rank] = jnp.where(bit == 1, a * C + me, -1)
            rank = rank + bit
    small = [
        pltpu.make_async_copy(cols_smem, cols_ref, small_sem.at[0]),
        pltpu.make_async_copy(start_smem, start_ref, small_sem.at[1]),
    ]
    for cp in small:
        cp.start()
    for i in range(PB):
        acc[...] = jnp.zeros_like(acc)
        for g in range(C):
            for s in range(KG):
                e = g * KG + s
                k = meta_ref[base + i * C * KG + e]
                lhs = left_ref[g, i * KG + s]
                for t in range(KG):
                    o = meta_ref[(i * C * KG + e) * KG + t]
                    acc[o] += jnp.dot(lhs, win_ref[k, t], preferred_element_type=jnp.float32)
        for o in range(classes):
            rows[i, o] = acc[o].astype(rows.dtype)
        store(i).start()
    for cp in small:
        cp.wait()
    for i in range(PB):
        fill(i).wait()
        store(i).wait()


def fast_on_device(blocks, block_cols):
    R, C = lax.axis_size("rows"), lax.axis_size("cols")
    PB, KG, BS = block_cols.shape[0], block_cols.shape[2], blocks.shape[-1]
    sizes = (R, C, PB, KG)
    slots = C * KG * KG
    vm = pl.BlockSpec(memory_space=pltpu.VMEM)
    hbm = pl.BlockSpec(memory_space=pltpu.HBM)
    sm = pl.BlockSpec(memory_space=pltpu.SMEM)
    dma = pltpu.SemaphoreType.DMA
    win, left, meta = pl.pallas_call(
        functools.partial(gather_kernel, sizes),
        out_shape=(
            jax.ShapeDtypeStruct((R, PB * KG, BS, BS), blocks.dtype),
            jax.ShapeDtypeStruct((C, PB * KG, BS, BS), blocks.dtype),
            jax.ShapeDtypeStruct((PB * slots + PB * C * KG + 2 * PB,), jnp.int32),
        ),
        in_specs=[hbm, hbm],
        out_specs=(vm, vm, sm),
        scratch_shapes=[
            pltpu.VMEM((R, C, KG, 1, PB), jnp.int32),
            pltpu.SMEM((R, C, KG, 1, PB), jnp.int32),
            pltpu.SMEM((R * PB,), jnp.int32),
            dma((R, len(SPANS))), dma((3, R, len(SPANS))), dma((C,)), dma((C,)),
            dma((R,)), dma((3, R)), dma((C,)), dma((3,)), dma((4,)),
        ],
        compiler_params=pltpu.CompilerParams(
            collective_id=0, has_side_effects=True, vmem_limit_bytes=VMEM_LIMIT
        ),
    )(
        pltpu.with_memory_space_constraint(blocks.reshape(PB * KG, BS, BS), pltpu.HBM),
        pltpu.with_memory_space_constraint(jnp.transpose(block_cols, (2, 1, 0)), pltpu.HBM),
    )
    out, cols, start = pl.pallas_call(
        functools.partial(square_kernel, sizes),
        out_shape=(
            pltpu.HBM((PB, 1, slots, BS, BS), blocks.dtype),
            pltpu.HBM((PB, 1, slots), jnp.int32),
            pltpu.HBM((1, PB), jnp.int32),
        ),
        in_specs=[sm, vm, vm],
        out_specs=(hbm, hbm, hbm),
        scratch_shapes=[
            pltpu.VMEM((R * PB // C, BS, BS), jnp.float32),
            pltpu.VMEM((slots - R * PB // C, BS, BS), blocks.dtype),
            pltpu.VMEM((PB, R * PB // C, BS, BS), blocks.dtype),
            pltpu.SMEM((PB, 1, slots), jnp.int32),
            pltpu.SMEM((1, PB), jnp.int32),
            dma((PB,)), dma((PB,)), dma((2,)),
        ],
        compiler_params=pltpu.CompilerParams(vmem_limit_bytes=VMEM_LIMIT),
    )(meta, left, win.reshape(R * PB, KG, BS, BS))
    return out, cols, start.T


def solution(mesh):
    in_specs = (P("rows", "cols", None, None, None), P("rows", "cols", None))
    out_specs = (P("rows", "cols", None, None, None), P("rows", "cols", None), P("rows", "cols"))
    body = fast_on_device if mesh.shape["rows"] == 2 * HP else on_device
    return jax.shard_map(
        body, mesh=mesh, in_specs=in_specs, out_specs=out_specs, check_vma=False
    )
```
